32 devices in a mesh: rows: 8 (over z, y), grp: 4 (over x, core).
Axes of the slice: x: 2, y: 2, z: 4, core: 2. Of those that a mesh axis runs over, the one named last changes fastest.
Arguments:
- table: float32 [65536, 256], P(('rows', 'grp')), may hold values from -1.5 to 1.5
- hot_slot: int32 [512], P(('rows', 'grp')), may hold values from 0 to 2047, as said below
- cold_row: int32 [32, 32, 64], P(('rows', 'grp')), may hold values from 0 to 2047, as said below
- cold_bag: int32 [32, 32, 64], P(('rows', 'grp')), may hold values from 0 to 511
- hot_pick: int32 [8192, 8], P(('rows', 'grp')), may hold values from 0 to 511
- dense: float32 [8192, 256], P(('rows', 'grp')), may hold values from -6 to 6
- label: int32 [8192], P(('rows', 'grp')), may hold values 0 or 1
Outputs:
- pooled: float32 [8192, 256], P(('rows', 'grp'))
- new_table: float32 [65536, 256], P(('rows', 'grp'))
- hot_new: float32 [512, 256], replicated
The draws below stay inside these ranges and needn't reach their ends.
Inputs may be any that keep to these rules, and one draw needn't show every extreme that they name: `hot_slot`: distinct within each device's block of 16 entries; hot row h lies in the shard of device h // 16. `cold_row`: a cold slot never names a hot row of its owner. `cold_bag`: a value of 256 or more marks an empty slot.
All inputs are finite; a program needn't handle non-finite values. No bound on the sum of `label` on one device may be relied on, other than what follows from the above.
Results may differ from the reference program's by a relative error of at most 0.0029.
Values may be sent and summed in bfloat16 or wider, within the bound.
No kernel may reach another device: no remote copies, remote signals or barrier semaphores. Data moves between devices by JAX's collectives and lax.ppermute only.
A program may use at most 64 MiB of HBM per device.

```python
import jax
import jax.numpy as jnp
from jax import lax

DIM = 256
ROWS_DEV = 2048
HOT_DEV = 16
B_DEV = 256
HBAG = 8
CAP = 64
TABLE_ROWS = 65536
HOT = 512
BATCH = 8192
DEVICES = 32


def shard_orders(key):
    keys = jax.random.split(jax.random.fold_in(key, 7), DEVICES)
    return jax.vmap(lambda k: jax.random.permutation(k, ROWS_DEV))(keys).astype(jnp.int32)


def draw_hot_slot(key, part):
    orders = shard_orders(key)
    return orders[:, :HOT_DEV].reshape(HOT).astype(jnp.int32)


def draw_cold_row(key, part):
    orders = shard_orders(key)
    picks = jax.random.randint(jax.random.fold_in(key, 11), (DEVICES, DEVICES, CAP), 0, ROWS_DEV - HOT_DEV) + HOT_DEV

    def one_source(pick):
        return jnp.take_along_axis(orders, pick, axis=1)
    return jax.vmap(one_source)(picks).astype(jnp.int32)


def with_ends(values, own_key, low, high):
    extent = values.shape
    place = [jax.random.randint(jax.random.fold_in(own_key, axis), (), 0, extent[axis]) for axis in range(len(extent))]
    values = values.at[tuple(place)].set(low)
    longest = extent.index(max(extent))
    place[longest] = (place[longest] + 1) % extent[longest]
    return values.at[tuple(place)].set(high)


def steps_of(rng, dims, shards, least, top_value):
    def one(dim, blocks):
        heights = jax.random.uniform(jax.random.fold_in(jax.random.fold_in(rng, 6), dim), (blocks,), jnp.float32, least / len(shards), top_value / len(shards))
        return jnp.repeat(jnp.exp(heights), dims[dim] // blocks).reshape((-1,) + (1,) * (len(dims) - dim - 1))

    gain = one(*shards[0])
    for cut in shards[1:]:
        gain = gain * one(*cut)
    return gain


def noise(rng, shape, width, most, shards=(), kind=jnp.bfloat16):
    result = width * jax.random.normal(rng, shape, jnp.float32)
    if shards:
        result = result * steps_of(rng, shape, shards, -0.22, 0.18)
    return jnp.clip(result, -most, most).astype(kind)


def setup_inputs(seed: int = 0) -> dict:
    seeds = jax.random.split(jax.random.key(seed), 8)
    return {
        "table": noise(seeds[0], (TABLE_ROWS, DIM), 0.25, 1.5, ((0, 32),), jnp.float32),
        "hot_slot": draw_hot_slot(jax.random.fold_in(seeds[7], 71), 0),
        "cold_row": draw_cold_row(jax.random.fold_in(seeds[7], 71), 0),
        "cold_bag": with_ends(jax.random.randint(seeds[3], (DEVICES, DEVICES, CAP), 0, 2 * B_DEV), jax.random.fold_in(seeds[3], 1), 0, (2 * B_DEV) - 1).astype(jnp.int32),
        "hot_pick": with_ends(jax.random.randint(seeds[4], (BATCH, HBAG), 0, HOT), jax.random.fold_in(seeds[4], 1), 0, HOT - 1).astype(jnp.int32),
        "dense": noise(seeds[5], (BATCH, DIM), 1.0, 6.0, ((0, 32),), jnp.float32),
        "label": with_ends((jax.random.randint(seeds[6], (BATCH,), 0, 2) < 1).astype(jnp.int32), jax.random.fold_in(seeds[6], 1), 0, 1),
    }


def reference(table, hot_slot, cold_row, cold_bag, hot_pick, dense, label):
    rounded = table.astype(jnp.bfloat16)
    owners = jnp.arange(DEVICES, dtype=jnp.int32)
    cold_id = (owners * ROWS_DEV)[None, :, None] + cold_row
    hot_id = (jnp.arange(HOT, dtype=jnp.int32) // HOT_DEV) * ROWS_DEV + hot_slot
    samples = jnp.arange(B_DEV, dtype=jnp.int32)

    def pool_one(args):
        ids, bags = args
        emb = rounded[ids.reshape(-1)]
        onehot = (samples[:, None] == bags.reshape(-1)[None, :]).astype(jnp.bfloat16)
        return jnp.dot(onehot, emb, preferred_element_type=jnp.float32)

    cold_pooled = lax.map(pool_one, (cold_id, cold_bag)).reshape(BATCH, DIM)
    hot_rows = rounded[hot_id]
    hot_pooled = jnp.sum(hot_rows[hot_pick].astype(jnp.float32), axis=1)
    pooled = cold_pooled + hot_pooled
    score = jnp.sum(pooled * dense, axis=1) / (DIM ** 0.5)
    err = jax.nn.sigmoid(score) - label.astype(jnp.float32)
    grad = err[:, None] * dense
    live = cold_bag < B_DEV
    source = (jnp.arange(DEVICES, dtype=jnp.int32) * B_DEV)[:, None, None]
    index = source + jnp.minimum(cold_bag, B_DEV - 1)
    table_grad = jnp.zeros((TABLE_ROWS, DIM), jnp.float32)

    def add_source(acc, args):
        idx, alive, ids = args
        slot_grad = jnp.where(alive.reshape(-1)[:, None], grad[idx.reshape(-1)], 0.0)
        return acc.at[ids.reshape(-1)].add(slot_grad), None

    table_grad, _ = lax.scan(add_source, table_grad, (index, live, cold_id))
    picked = hot_id[hot_pick].reshape(-1)
    spread = jnp.repeat(grad, HBAG, axis=0)
    table_grad = table_grad.at[picked].add(spread)
    new_table = table - 0.1 * table_grad
    hot_new = new_table[hot_id]
    return pooled, new_table, hot_new
```

```python
import jax
import jax.numpy as jnp
from jax import lax
from jax.sharding import PartitionSpec as P

AXES = ("rows", "grp")


def exchange(x):
    return lax.all_to_all(x, AXES, split_axis=0, concat_axis=0, tiled=True)


def body(table, hot_slot, cold_row, cold_bag, hot_pick, dense, label):
    width = table.shape[1]
    samples = dense.shape[0]
    own_hot = hot_slot.shape[0]
    peers, per_peer = cold_row.shape[1], cold_row.shape[2]
    slots = peers * per_peer
    bf16 = jnp.bfloat16
    arrived = exchange(cold_row[0]).reshape(slots)
    rounded = table.astype(bf16)
    owned = jnp.arange(table.shape[0], dtype=jnp.int32)
    looked = rounded[arrived].reshape(peers, per_peer, width)
    hot_rows = table[hot_slot]
    shared = jnp.broadcast_to(hot_rows.astype(bf16)[None], (peers, own_hot, width))
    returned = exchange(jnp.concatenate([looked, shared], axis=1))
    cold_rows = returned[:, :per_peer].reshape(slots, width)
    hot_copy = returned[:, per_peer:].reshape(peers * own_hot, width)
    bags = cold_bag[0].reshape(slots)
    selector = (jnp.arange(samples, dtype=jnp.int32)[:, None] == bags[None, :]).astype(bf16)
    hot_total = peers * own_hot
    picks = jnp.sum(
        (hot_pick[:, :, None] == jnp.arange(hot_total, dtype=jnp.int32)).astype(jnp.float32), axis=1
    ).astype(bf16)
    pooled = jnp.dot(selector, cold_rows, preferred_element_type=jnp.float32) + jnp.dot(
        picks, hot_copy, preferred_element_type=jnp.float32
    )
    score = jnp.sum(pooled * dense, axis=1) / width**0.5
    err = jax.nn.sigmoid(score) - label.astype(jnp.float32)
    grad = (err[:, None] * dense).astype(bf16)
    over_samples = (((0,), (0,)), ((), ()))
    slot_grad = lax.dot_general(selector, grad, over_samples, preferred_element_type=jnp.float32)
    hot_part = lax.dot_general(picks, grad, over_samples, preferred_element_type=jnp.float32)
    sent = jnp.concatenate(
        [
            slot_grad.astype(bf16).reshape(peers, per_peer, width),
            hot_part.astype(bf16).reshape(peers, own_hot, width),
        ],
        axis=1,
    )
    delivered = exchange(sent)
    own_grad = jnp.sum(delivered[:, per_peer:].astype(jnp.float32), axis=0)
    placed = (owned[:, None] == arrived[None, :]).astype(bf16)
    table_grad = jnp.dot(
        placed, delivered[:, :per_peer].reshape(slots, width), preferred_element_type=jnp.float32
    )
    own_new = hot_rows - 0.1 * own_grad
    new_table = (table - 0.1 * table_grad).at[hot_slot].set(own_new)
    hot_new = exchange(jnp.broadcast_to(own_new[None], (peers, own_hot, width)))
    return (pooled, new_table, hot_new.reshape(hot_total, width))


def solution(mesh):
    placed = (
        P(AXES, None),
        P(AXES),
        P(AXES, None, None),
        P(AXES, None, None),
        P(AXES, None),
        P(AXES, None),
        P(AXES),
    )
    return jax.shard_map(
        body,
        mesh=mesh,
        in_specs=placed,
        out_specs=(P(AXES, None), P(AXES, None), P()),
        check_vma=False,
    )
```

```python
import jax
import jax.numpy as jnp
from jax import lax
from jax.experimental import pallas as pl
from jax.experimental.pallas import tpu as pltpu
from jax.sharding import PartitionSpec as P


AXES = ("rows", "grp")
LANES = 128
MIB = 1 << 20
BF16 = jnp.bfloat16
F32 = jnp.float32
I32 = jnp.int32


def exchange(x):
    return lax.all_to_all(x, AXES, split_axis=0, concat_axis=0, tiled=True)


def column(row):
    return jnp.transpose(jnp.broadcast_to(row, (LANES, LANES)))


def lane_iota(shape):
    return lax.broadcasted_iota(I32, shape, 1)


def one_hot(mask):
    return jnp.where(mask, 1.0, 0.0).astype(BF16)


def packed_row(ref, at, per_peer, part):
    row = None
    for j in range(LANES // per_peer):
        shift = (j - part) * per_peer % LANES
        other = ref[at(j)]
        other = pltpu.roll(other, shift, 1) if shift else other
        row = other if row is None else jnp.where(lane_iota(row.shape) < j * per_peer, row, other)
    return row


def mark_of(ids):
    return ((LANES + (ids & (LANES - 1))) << (ids >> 7)).astype(F32).astype(BF16)


def fetch(pairs, sems):
    copies = [pltpu.make_async_copy(a, b, sems.at[k]) for k, (a, b) in enumerate(pairs)]
    for copy in copies:
        copy.start()
    return copies


def offsets(chunks):
    return [sum(chunk.shape[0] for chunk in chunks[:k]) for k in range(len(chunks))]


def prepare_kernel(
    slot_ref, table_hbm, dense_hbm, pick_hbm, packed_ref, hot_ref, dense_ref, pick_ref, sems
):
    own_hot = slot_ref.shape[0]
    dense_in, pick_in, *rows_in = fetch(
        [(dense_hbm, dense_ref), (pick_hbm, pick_ref)]
        + [
            (table_hbm.at[pl.ds(slot_ref[k], 1)], hot_ref.at[pl.ds(k, 1)])
            for k in range(own_hot)
        ],
        sems,
    )
    samples = dense_ref.shape[0]
    dense_in.wait()
    packed_ref[:samples, :] = dense_ref[...].astype(BF16)
    pick_in.wait()
    packed_ref[samples + 2 * own_hot :, :] = mark_of(pick_ref[...])
    for row_in in rows_in:
        row_in.wait()
    hot = hot_ref[...]
    high = hot.astype(BF16)
    packed_ref[samples : samples + own_hot, :] = high
    packed_ref[samples + own_hot : samples + 2 * own_hot, :] = (hot - high.astype(F32)).astype(BF16)


def lookup_kernel(request_ref, table_ref, out_ref):
    peers = request_ref.shape[0]
    rows = table_ref.shape[0]
    per_peer = request_ref.shape[2] // 2
    group = LANES // per_peer
    tile = 4
    table = table_ref[...].astype(BF16)
    for first in range(0, peers // group, tile):
        pieces = []
        for k in range(first, first + tile):
            wanted = column(packed_row(request_ref, lambda j: k * group + j, per_peer, 0))
            pieces.append(
                jnp.concatenate(
                    [one_hot(wanted == lane_iota(wanted.shape) + c) for c in range(0, rows, LANES)],
                    axis=1,
                )
            )
        hits = jnp.concatenate(pieces, axis=0)
        out_ref[first * LANES : (first + tile) * LANES, :] = jnp.dot(
            hits, table, preferred_element_type=F32
        ).astype(BF16)


def marks_kernel(source_ref, me_ref, request_ref, *refs):
    *chunks, hot_ref, cold_ref, pick_ref, sems = refs
    per_peer = request_ref.shape[2] // 2
    samples = cold_ref.shape[1]
    own_hot = 2 * hot_ref.shape[0] // request_ref.shape[0]
    first = samples + 2 * own_hot
    picks_in = fetch(
        [
            (chunk.at[:, first:], pick_ref.at[pl.ds(n, chunk.shape[0])])
            for n, chunk in zip(offsets(chunks), chunks)
        ],
        sems,
    )
    one, zero = jnp.ones((), BF16), jnp.zeros((), BF16)
    for n in range(request_ref.shape[0]):
        bags = column(request_ref[source_ref[n]])[per_peer:]
        at = n * per_peer
        for c in range(0, samples, LANES):
            cold_ref[at : at + per_peer, c : c + LANES] = one_hot(bags == lane_iota(bags.shape) + c)
    rows = lax.broadcasted_iota(I32, (hot_ref.shape[0], LANES), 0)
    odd = me_ref[0] & 1
    ids = mark_of(rows + (rows // own_hot + odd) * own_hot)
    for arrived in picks_in:
        arrived.wait()
    for n in range(pick_ref.shape[0]):
        for c in range(0, samples, LANES):
            total = None
            for j in range(pick_ref.shape[1]):
                hit = jnp.where(ids == pick_ref[n, j : j + 1, c : c + LANES], one, zero)
                total = hit if total is None else total + hit
            at = n * samples + c
            hot_ref[:, at : at + LANES] = total


def pool_kernel(source_ref, rows_ref, bag_hbm, pick_hbm, dense_hbm, label_hbm, *refs):
    *chunks, pooled_ref, err_ref, hot_ref, near_ref, bag_ref, pick_ref, dense_ref, label_ref, sems = refs
    samples, width = dense_ref.shape
    hot_total = hot_ref.shape[0]
    own_hot = hot_total // err_ref.shape[0]
    high = slice(samples, samples + own_hot)
    bag_in, pick_in, dense_in, label_in, *hot_in = fetch(
        [
            (bag_hbm, bag_ref),
            (pick_hbm, pick_ref),
            (dense_hbm, dense_ref),
            (label_hbm, label_ref),
        ]
        + [
            (chunk.at[:, high], near_ref.at[pl.ds(n, chunk.shape[0])])
            for n, chunk in zip(offsets(chunks), chunks)
        ],
        sems,
    )
    bag_in.wait()
    ids = lax.broadcasted_iota(I32, (samples, LANES), 0)
    chosen = jnp.concatenate(
        [one_hot(ids == bag_ref[k : k + 1, :]) for k in range(bag_ref.shape[0])], axis=1
    )
    pooled = jnp.dot(chosen, rows_ref[...], preferred_element_type=F32)
    pick_in.wait()
    counts = []
    for h in range(0, hot_total, LANES):
        ids = lax.broadcasted_iota(I32, (LANES, samples), 0) + h
        total = jnp.zeros((LANES, samples), F32)
        for j in range(pick_ref.shape[0]):
            total = total + jnp.where(ids == pick_ref[j : j + 1, :], 1.0, 0.0)
        counts.append(total.astype(BF16))
    for arrived in hot_in:
        arrived.wait()
    for n in range(near_ref.shape[0]):
        at = pl.multiple_of(source_ref[n] * own_hot, own_hot)
        hot_ref[pl.ds(at, own_hot), :] = near_ref[n]
    pooled = pooled + lax.dot_general(
        jnp.concatenate(counts, axis=0),
        hot_ref[...],
        (((0,), (0,)), ((), ())),
        preferred_element_type=F32,
    )
    pooled_ref[...] = pooled
    dense_in.wait()
    label_in.wait()
    score = jnp.sum(pooled * dense_ref[...], axis=1, keepdims=True) / width**0.5
    flat = jnp.transpose(jnp.broadcast_to(score, (samples, LANES)))[:1, :]
    err = 1.0 / (1.0 + jnp.exp(-flat)) - label_ref[...].astype(F32)
    err_ref[...] = jnp.broadcast_to(err[None], err_ref.shape)


def hot_kernel(source_ref, me_ref, marks_ref, err_ref, *refs):
    *chunks, new_ref, grad_ref = refs
    hot_half, _ = new_ref.shape
    peers = err_ref.shape[0]
    samples = err_ref.shape[2]
    own_hot = 2 * hot_half // peers
    total, n = None, 0
    for chunk in chunks:
        parts = chunk.shape[0]
        errs = [err_ref[source_ref[n + p]].astype(BF16) for p in range(parts)]
        near = jnp.dot(
            marks_ref[:, n * samples : (n + parts) * samples] * jnp.concatenate(errs, axis=1),
            jnp.concatenate([chunk[p, :samples, :] for p in range(parts)], axis=0),
            preferred_element_type=F32,
        )
        total = near if total is None else total + near
        n += parts
    grad_ref[...] = total
    odd = me_ref[0] & 1
    n = 0
    for chunk in chunks:
        for p in range(chunk.shape[0]):
            owner = source_ref[n]

            @pl.when((owner & 1) == odd)
            def _():
                at = pl.multiple_of((owner // 2) * own_hot, own_hot)
                old = chunk[p, samples : samples + own_hot, :].astype(F32)
                old = old + chunk[p, samples + own_hot : samples + 2 * own_hot, :].astype(F32)
                new_ref[pl.ds(at, own_hot), :] = old - 0.1 * grad_ref[pl.ds(at, own_hot), :]

            n += 1


def cold_kernel(
    source_ref, slot_ref, me_ref, cold_ref, err_ref, request_ref, table_ref, hot_ref, *refs
):
    *chunks, new_ref, slots_ref = refs
    rows = table_ref.shape[0]
    peers = request_ref.shape[0]
    samples = cold_ref.shape[1]
    per_peer = request_ref.shape[2] // 2
    own_hot = slot_ref.shape[0]
    n = 0
    for chunk in chunks:
        for p in range(chunk.shape[0]):
            at = n * per_peer
            part = jnp.dot(
                cold_ref[at : at + per_peer, :] * err_ref[source_ref[n]].astype(BF16),
                chunk[p, :samples, :],
                preferred_element_type=F32,
            )
            slots_ref[at : at + per_peer, :] = part.astype(BF16)
            n += 1
    group = LANES // per_peer
    packed = [
        packed_row(request_ref, lambda j: source_ref[n + j], per_peer, 0)
        for n in range(0, peers, group)
    ]
    chunk_rows = 256
    ids = lax.broadcasted_iota(I32, (chunk_rows, LANES), 0)
    for r in range(0, rows, chunk_rows):
        place = jnp.concatenate([one_hot(ids + r == row) for row in packed], axis=1)
        moved = jnp.dot(place, slots_ref[...], preferred_element_type=F32)
        new_ref[r : r + chunk_rows, :] = table_ref[r : r + chunk_rows, :] - 0.1 * moved
    base = (me_ref[0] // 2) * own_hot
    for k in range(own_hot):
        new_ref[pl.ds(slot_ref[k], 1), :] = hot_ref[pl.ds(base + k, 1), :]


def gather_all(x, devices):
    def swap(held, mask):
        return lax.ppermute(held, AXES, [(i, i ^ mask(i)) for i in range(devices)])

    first = lambda i: 2 if i & 1 else 4
    second = lambda i: 4 if i & 1 else 2
    other = lambda i: 1
    deep = [swap(x, lambda i: mask) for mask in deep_masks(devices)]
    near = [x, swap(x, first), swap(x, second)]
    near = jnp.concatenate(near + [swap(near[1], second)], axis=0)
    own = jnp.concatenate(deep, axis=0)
    across = swap(own, first)
    up = swap(own, second)
    held = [near, own, across, up, swap(across, second)]
    return held + [swap(chunk, other) for chunk in held]


def deep_masks(devices):
    masks = [0]
    for b in range(devices.bit_length() - 2, 2, -1):
        masks += [mask | 1 << b for mask in masks]
    return masks[1:]


def sources_of(me, devices):
    deep = deep_masks(devices)

    def half(owner):
        first = jnp.where(owner & 1 == 1, 2, 4)
        turns = [0, first, 6 - first, 6]
        return [owner ^ turn for turn in turns] + [owner ^ turn ^ m for turn in turns for m in deep]

    return jnp.stack(half(me) + half(me ^ 1)).astype(I32)


def gathered_body(table, hot_slot, cold_row, cold_bag, hot_pick, dense, label):
    rows, width = table.shape
    samples = dense.shape[0]
    own_hot = hot_slot.shape[0]
    peers, per_peer = cold_row.shape[1], cold_row.shape[2]
    slots = peers * per_peer
    hot_total = peers * own_hot
    me = lax.axis_index(AXES).astype(I32)
    source = sources_of(me, peers)

    def shape(*dims, kind=BF16):
        return jax.ShapeDtypeStruct(dims, kind)

    def call(kernel, out_shape, where, inputs, mib, flops, scratch):
        spaces = {"s": pltpu.SMEM, "v": pltpu.VMEM, "h": pltpu.HBM}
        specs = [pl.BlockSpec(memory_space=spaces[w]) for w in where]
        return pl.pallas_call(
            kernel,
            out_shape=out_shape,
            in_specs=specs[: len(inputs)],
            out_specs=tuple(specs[len(inputs) :]),
            scratch_shapes=scratch,
            compiler_params=pltpu.CompilerParams(vmem_limit_bytes=mib * MIB),
            cost_estimate=pl.CostEstimate(flops=flops, bytes_accessed=4 * MIB, transcendentals=0),
        )(*inputs)

    def copies(count):
        return pltpu.SemaphoreType.DMA((count,))

    request = exchange(jnp.concatenate([cold_row[0], cold_bag[0]], axis=1)[:, None, :])
    part_rows = samples + 2 * own_hot + hot_pick.shape[1]
    work = slots * rows * width
    picks = hot_pick.T
    bags = cold_bag.reshape(slots // LANES, LANES)
    (packed,) = call(
        prepare_kernel,
        (shape(part_rows, width),),
        "shhhv",
        [hot_slot, table, dense, picks],
        63,
        work,
        [
            pltpu.VMEM((own_hot, width), F32),
            pltpu.VMEM((samples, width), F32),
            pltpu.VMEM(picks.shape, I32),
            copies(2 + own_hot),
        ],
    )
    chunks = gather_all(packed[None], peers)
    many = "v" * len(chunks)
    (looked,) = call(
        lookup_kernel, (shape(slots, width),), "vvv", [request, table], 24, 2 * work, []
    )
    returned = exchange(looked.reshape(peers, per_peer, width)).reshape(slots, width)
    pooled, err = call(
        pool_kernel,
        (shape(samples, width, kind=F32), shape(peers, 1, samples, kind=F32)),
        "svhhhh" + "h" * len(chunks) + "vv",
        [source, returned, bags, picks, dense, label.reshape(1, samples)] + chunks,
        24,
        work,
        [
            pltpu.VMEM((hot_total, width), BF16),
            pltpu.VMEM((peers, own_hot, width), BF16),
            pltpu.VMEM(bags.shape, I32),
            pltpu.VMEM(picks.shape, I32),
            pltpu.VMEM((samples, width), F32),
            pltpu.VMEM((1, samples), I32),
            copies(4 + len(chunks)),
        ],
    )
    errs = exchange(err)
    marks, cold = call(
        marks_kernel,
        (shape(hot_total // 2, peers * samples), shape(slots, samples)),
        "ssv" + "h" * len(chunks) + "vv",
        [source, me[None], request] + chunks,
        24,
        4 * work,
        [pltpu.VMEM((peers, hot_pick.shape[1], samples), BF16), copies(len(chunks))],
    )
    (hot_here,) = call(
        hot_kernel,
        (shape(hot_total // 2, width, kind=F32),),
        "ssvv" + many + "v",
        [source, me[None], marks, errs] + chunks,
        24,
        work,
        [pltpu.VMEM((hot_total // 2, width), F32)],
    )
    hot_there = lax.ppermute(hot_here, AXES, [(i, i ^ 1) for i in range(peers)])
    (new_table,) = call(
        cold_kernel,
        (shape(rows, width, kind=F32),),
        "sssvvvvv" + many + "v",
        [source, hot_slot, me[None], cold, errs, request, table, hot_here] + chunks,
        24,
        4 * work,
        [pltpu.VMEM((slots, width), BF16)],
    )
    split = (peers // 2, 1, own_hot, width)
    here, there = hot_here.reshape(split), hot_there.reshape(split)
    odd = (me & 1) == 1
    hot_new = jnp.concatenate([jnp.where(odd, there, here), jnp.where(odd, here, there)], axis=1)
    hot_new = hot_new.reshape(hot_total, width)
    return (pooled, new_table, hot_new)


def exchanged_body(table, hot_slot, cold_row, cold_bag, hot_pick, dense, label):
    width = table.shape[1]
    samples = dense.shape[0]
    own_hot = hot_slot.shape[0]
    peers, per_peer = cold_row.shape[1], cold_row.shape[2]
    slots = peers * per_peer
    bf16 = BF16
    arrived = exchange(cold_row[0]).reshape(slots)
    rounded = table.astype(bf16)
    owned = jnp.arange(table.shape[0], dtype=jnp.int32)
    looked = rounded[arrived].reshape(peers, per_peer, width)
    hot_rows = table[hot_slot]
    shared = jnp.broadcast_to(hot_rows.astype(bf16)[None], (peers, own_hot, width))
    returned = exchange(jnp.concatenate([looked, shared], axis=1))
    cold_rows = returned[:, :per_peer].reshape(slots, width)
    hot_copy = returned[:, per_peer:].reshape(peers * own_hot, width)
    bags = cold_bag[0].reshape(slots)
    selector = (jnp.arange(samples, dtype=jnp.int32)[:, None] == bags[None, :]).astype(bf16)
    hot_total = peers * own_hot
    picks = jnp.sum(
        (hot_pick[:, :, None] == jnp.arange(hot_total, dtype=jnp.int32)).astype(jnp.float32), axis=1
    ).astype(bf16)
    pooled = jnp.dot(selector, cold_rows, preferred_element_type=jnp.float32) + jnp.dot(
        picks, hot_copy, preferred_element_type=jnp.float32
    )
    score = jnp.sum(pooled * dense, axis=1) / width**0.5
    err = jax.nn.sigmoid(score) - label.astype(jnp.float32)
    grad = (err[:, None] * dense).astype(bf16)
    over_samples = (((0,), (0,)), ((), ()))
    slot_grad = lax.dot_general(selector, grad, over_samples, preferred_element_type=jnp.float32)
    hot_part = lax.dot_general(picks, grad, over_samples, preferred_element_type=jnp.float32)
    sent = jnp.concatenate(
        [
            slot_grad.astype(bf16).reshape(peers, per_peer, width),
            hot_part.astype(bf16).reshape(peers, own_hot, width),
        ],
        axis=1,
    )
    delivered = exchange(sent)
    own_grad = jnp.sum(delivered[:, per_peer:].astype(jnp.float32), axis=0)
    placed = (owned[:, None] == arrived[None, :]).astype(bf16)
    table_grad = jnp.dot(
        placed, delivered[:, :per_peer].reshape(slots, width), preferred_element_type=jnp.float32
    )
    own_new = hot_rows - 0.1 * own_grad
    new_table = (table - 0.1 * table_grad).at[hot_slot].set(own_new)
    hot_new = exchange(jnp.broadcast_to(own_new[None], (peers, own_hot, width)))
    return (pooled, new_table, hot_new.reshape(hot_total, width))


def solution(mesh):
    placed = (
        P(AXES, None),
        P(AXES),
        P(AXES, None, None),
        P(AXES, None, None),
        P(AXES, None),
        P(AXES, None),
        P(AXES),
    )
    devices = mesh.shape["rows"] * mesh.shape["grp"]

    def body(*blocks):
        _, hot_slot, cold_row, _, _, dense, _ = blocks
        samples, own_hot = dense.shape[0], hot_slot.shape[0]
        marks = 2 * devices * samples * devices * own_hot
        fits = marks <= 16 * MIB and 2 * cold_row.shape[2] == LANES
        fits = fits and devices & (devices - 1) == 0 and devices >= 16 and devices * own_hot <= 64 * LANES
        return (gathered_body if fits else exchanged_body)(*blocks)

    return jax.shard_map(
        body,
        mesh=mesh,
        in_specs=placed,
        out_specs=(P(AXES, None), P(AXES, None), P()),
        check_vma=False,
    )
```

```python
import jax
import jax.numpy as jnp
from jax import lax
from jax.experimental import pallas as pl
from jax.experimental.pallas import tpu as pltpu
from jax.sharding import PartitionSpec as P


AXES = ("rows", "grp")
LANES = 128
MIB = 1 << 20
BF16 = jnp.bfloat16
F32 = jnp.float32
I32 = jnp.int32


def exchange(x):
    return lax.all_to_all(x, AXES, split_axis=0, concat_axis=0, tiled=True)


def column(row):
    return jnp.transpose(jnp.broadcast_to(row, (LANES, LANES)))


def lane_iota(shape):
    return lax.broadcasted_iota(I32, shape, 1)


def one_hot(mask):
    return jnp.where(mask, 1.0, 0.0).astype(BF16)


def packed_row(ref, at, per_peer, part):
    row = None
    for j in range(LANES // per_peer):
        shift = (j - part) * per_peer % LANES
        other = ref[at(j)]
        other = pltpu.roll(other, shift, 1) if shift else other
        row = other if row is None else jnp.where(lane_iota(row.shape) < j * per_peer, row, other)
    return row


def mark_of(ids):
    return ((LANES + (ids & (LANES - 1))) << (ids >> 7)).astype(F32).astype(BF16)


def fetch(pairs, sems):
    copies = [pltpu.make_async_copy(a, b, sems.at[k]) for k, (a, b) in enumerate(pairs)]
    for copy in copies:
        copy.start()
    return copies


def offsets(chunks):
    return [sum(chunk.shape[0] for chunk in chunks[:k]) for k in range(len(chunks))]


def prepare_kernel(
    slot_ref, table_hbm, dense_hbm, pick_hbm, packed_ref, hot_ref, dense_ref, pick_ref, sems
):
    own_hot = slot_ref.shape[0]
    dense_in, pick_in, *rows_in = fetch(
        [(dense_hbm, dense_ref), (pick_hbm, pick_ref)]
        + [
            (table_hbm.at[pl.ds(slot_ref[k], 1)], hot_ref.at[pl.ds(k, 1)])
            for k in range(own_hot)
        ],
        sems,
    )
    samples = dense_ref.shape[0]
    dense_in.wait()
    packed_ref[:samples, :] = dense_ref[...].astype(BF16)
    pick_in.wait()
    packed_ref[samples + 2 * own_hot :, :] = mark_of(pick_ref[...])
    for row_in in rows_in:
        row_in.wait()
    hot = hot_ref[...]
    high = hot.astype(BF16)
    packed_ref[samples : samples + own_hot, :] = high
    packed_ref[samples + own_hot : samples + 2 * own_hot, :] = (hot - high.astype(F32)).astype(BF16)


def lookup_kernel(request_ref, table_ref, out_ref):
    peers = request_ref.shape[0]
    rows = table_ref.shape[0]
    per_peer = request_ref.shape[2] // 2
    group = LANES // per_peer
    tile = 4
    table = table_ref[...].astype(BF16)
    for first in range(0, peers // group, tile):
        pieces = []
        for k in range(first, first + tile):
            wanted = column(packed_row(request_ref, lambda j: k * group + j, per_peer, 0))
            pieces.append(
                jnp.concatenate(
                    [one_hot(wanted == lane_iota(wanted.shape) + c) for c in range(0, rows, LANES)],
                    axis=1,
                )
            )
        hits = jnp.concatenate(pieces, axis=0)
        out_ref[first * LANES : (first + tile) * LANES, :] = jnp.dot(
            hits, table, preferred_element_type=F32
        ).astype(BF16)


def marks_kernel(source_ref, me_ref, request_ref, *refs):
    *chunks, hot_ref, cold_ref, rows_ref, pick_ref, dense_ref, sems = refs
    per_peer = request_ref.shape[2] // 2
    samples = cold_ref.shape[1]
    own_hot = 2 * hot_ref.shape[0] // request_ref.shape[0]
    first = samples + 2 * own_hot
    picks_in = fetch(
        [
            (chunk.at[:, first:], pick_ref.at[pl.ds(n, chunk.shape[0])])
            for n, chunk in zip(offsets(chunks), chunks)
        ],
        sems,
    )
    dense_in = fetch(
        [
            (chunk.at[:, :samples], dense_ref.at[pl.ds(n, chunk.shape[0])])
            for n, chunk in zip(offsets(chunks), chunks)
        ],
        sems.at[pl.ds(len(chunks), len(chunks))],
    )
    one, zero = jnp.ones((), BF16), jnp.zeros((), BF16)
    for n in range(pick_ref.shape[0]):
        bags = column(request_ref[source_ref[n]])[per_peer:]
        at = n * per_peer
        for c in range(0, samples, LANES):
            cold_ref[at : at + per_peer, c : c + LANES] = one_hot(bags == lane_iota(bags.shape) + c)
    rows = lax.broadcasted_iota(I32, (hot_ref.shape[0], LANES), 0)
    odd = me_ref[0] & 1
    ids = mark_of(rows + (rows // own_hot + odd) * own_hot)
    for arrived in picks_in:
        arrived.wait()
    for n in range(pick_ref.shape[0]):
        for c in range(0, samples, LANES):
            total = None
            for j in range(pick_ref.shape[1]):
                hit = jnp.where(ids == pick_ref[n, j : j + 1, c : c + LANES], one, zero)
                total = hit if total is None else total + hit
            at = n * samples + c
            hot_ref[:, at : at + LANES] = total.astype(hot_ref.dtype)
    for arrived in dense_in:
        arrived.wait()
    for n in range(pick_ref.shape[0]):
        at = slice(n * per_peer, (n + 1) * per_peer)
        rows_ref[at, :] = jnp.dot(
            cold_ref[at, :], dense_ref[n], preferred_element_type=F32
        ).astype(BF16)


def pool_kernel(source_ref, rows_ref, bag_hbm, pick_hbm, dense_hbm, label_hbm, *refs):
    *chunks, pooled_ref, err_ref, hot_ref, near_ref, bag_ref, pick_ref, dense_ref, label_ref, sems = refs
    samples, width = dense_ref.shape
    hot_total = hot_ref.shape[0]
    own_hot = hot_total // err_ref.shape[0]
    high = slice(samples, samples + own_hot)
    bag_in, pick_in, dense_in, label_in, *hot_in = fetch(
        [
            (bag_hbm, bag_ref),
            (pick_hbm, pick_ref),
            (dense_hbm, dense_ref),
            (label_hbm, label_ref),
        ]
        + [
            (chunk.at[:, high], near_ref.at[pl.ds(n, chunk.shape[0])])
            for n, chunk in zip(offsets(chunks), chunks)
        ],
        sems,
    )
    bag_in.wait()
    ids = lax.broadcasted_iota(I32, (samples, LANES), 0)
    chosen = jnp.concatenate(
        [one_hot(ids == bag_ref[k : k + 1, :]) for k in range(bag_ref.shape[0])], axis=1
    )
    pooled = jnp.dot(chosen, rows_ref[...], preferred_element_type=F32)
    pick_in.wait()
    counts = []
    for h in range(0, hot_total, LANES):
        ids = lax.broadcasted_iota(I32, (LANES, samples), 0) + h
        total = jnp.zeros((LANES, samples), F32)
        for j in range(pick_ref.shape[0]):
            total = total + jnp.where(ids == pick_ref[j : j + 1, :], 1.0, 0.0)
        counts.append(total.astype(BF16))
    for arrived in hot_in:
        arrived.wait()
    for n in range(near_ref.shape[0]):
        at = pl.multiple_of(source_ref[n] * own_hot, own_hot)
        hot_ref[pl.ds(at, own_hot), :] = near_ref[n]
    pooled = pooled + lax.dot_general(
        jnp.concatenate(counts, axis=0),
        hot_ref[...],
        (((0,), (0,)), ((), ())),
        preferred_element_type=F32,
    )
    pooled_ref[...] = pooled
    dense_in.wait()
    label_in.wait()
    score = jnp.sum(pooled * dense_ref[...], axis=1, keepdims=True) / width**0.5
    flat = jnp.transpose(jnp.broadcast_to(score, (samples, LANES)))[:1, :]
    err = 1.0 / (1.0 + jnp.exp(-flat)) - label_ref[...].astype(F32)
    err_ref[...] = jnp.broadcast_to(err[None], err_ref.shape)


def hot_kernel(source_ref, me_ref, marks0_ref, marks1_ref, err_ref, *refs):
    *chunks, new_ref, grad_ref = refs
    hot_half, _ = new_ref.shape
    peers = err_ref.shape[0]
    samples = err_ref.shape[2]
    own_hot = 2 * hot_half // peers
    total, n = None, 0
    for chunk in chunks:
        parts = chunk.shape[0]
        errs = [err_ref[source_ref[n + p]].astype(BF16) for p in range(parts)]
        marks_ref, at = marks0_ref, n * samples
        if at >= marks0_ref.shape[1]:
            marks_ref, at = marks1_ref, at - marks0_ref.shape[1]
        near = jnp.dot(
            marks_ref[:, at : at + parts * samples].astype(BF16) * jnp.concatenate(errs, axis=1),
            jnp.concatenate([chunk[p, :samples, :] for p in range(parts)], axis=0),
            preferred_element_type=F32,
        )
        total = near if total is None else total + near
        n += parts
    grad_ref[...] = total
    odd = me_ref[0] & 1
    n = 0
    for chunk in chunks:
        for p in range(chunk.shape[0]):
            owner = source_ref[n]

            @pl.when((owner & 1) == odd)
            def _():
                at = pl.multiple_of((owner // 2) * own_hot, own_hot)
                old = chunk[p, samples : samples + own_hot, :].astype(F32)
                old = old + chunk[p, samples + own_hot : samples + 2 * own_hot, :].astype(F32)
                new_ref[pl.ds(at, own_hot), :] = old - 0.1 * grad_ref[pl.ds(at, own_hot), :]

            n += 1


def cold_kernel(
    source_ref, slot_ref, me_ref, cold0_ref, cold1_ref, rows0_ref, rows1_ref, err_ref, request_ref,
    table_ref, hot_ref, new_ref, slots_ref,
):
    rows = table_ref.shape[0]
    peers = request_ref.shape[0]
    per_peer = request_ref.shape[2] // 2
    own_hot = slot_ref.shape[0]
    early = cold0_ref.shape[0] // per_peer
    for n in range(peers):
        cold_ref, rows_ref, at = cold0_ref, rows0_ref, n * per_peer
        if n >= early:
            cold_ref, rows_ref, at = cold1_ref, rows1_ref, (n - early) * per_peer
        err = cold_ref[at : at + per_peer, :].astype(F32) * err_ref[source_ref[n]]
        err = jnp.sum(err, axis=1, keepdims=True)
        slots_ref[n * per_peer : (n + 1) * per_peer, :] = (
            err * rows_ref[at : at + per_peer, :].astype(F32)
        ).astype(BF16)
    group = LANES // per_peer
    packed = [
        packed_row(request_ref, lambda j: source_ref[n + j], per_peer, 0)
        for n in range(0, peers, group)
    ]
    chunk_rows = 256
    ids = lax.broadcasted_iota(I32, (chunk_rows, LANES), 0)
    for r in range(0, rows, chunk_rows):
        place = jnp.concatenate([one_hot(ids + r == row) for row in packed], axis=1)
        moved = jnp.dot(place, slots_ref[...], preferred_element_type=F32)
        new_ref[r : r + chunk_rows, :] = table_ref[r : r + chunk_rows, :] - 0.1 * moved
    base = (me_ref[0] // 2) * own_hot
    for k in range(own_hot):
        new_ref[pl.ds(slot_ref[k], 1), :] = hot_ref[pl.ds(base + k, 1), :]


def gather_all(x, devices):
    def swap(held, mask):
        return lax.ppermute(held, AXES, [(i, i ^ mask(i)) for i in range(devices)])

    first = lambda i: 2 if i & 1 else 4
    second = lambda i: 4 if i & 1 else 2
    other = lambda i: 1
    deep = [swap(x, lambda i: mask) for mask in deep_masks(devices)]
    near = [x, swap(x, first), swap(x, second)]
    near = jnp.concatenate(near + [swap(near[1], second)], axis=0)
    own = jnp.concatenate(deep, axis=0)
    across = swap(own, first)
    up = swap(own, second)
    held = [near, own, across, up, swap(across, second)]
    return held + [swap(chunk, other) for chunk in held]


def deep_masks(devices):
    masks = [0]
    for b in range(devices.bit_length() - 2, 2, -1):
        masks += [mask | 1 << b for mask in masks]
    return masks[1:]


def sources_of(me, devices):
    deep = deep_masks(devices)

    def half(owner):
        first = jnp.where(owner & 1 == 1, 2, 4)
        turns = [0, first, 6 - first, 6]
        return [owner ^ turn for turn in turns] + [owner ^ turn ^ m for turn in turns for m in deep]

    return jnp.stack(half(me) + half(me ^ 1)).astype(I32)


def gathered_body(table, hot_slot, cold_row, cold_bag, hot_pick, dense, label):
    rows, width = table.shape
    samples = dense.shape[0]
    own_hot = hot_slot.shape[0]
    peers, per_peer = cold_row.shape[1], cold_row.shape[2]
    slots = peers * per_peer
    hot_total = peers * own_hot
    me = lax.axis_index(AXES).astype(I32)
    source = sources_of(me, peers)

    def shape(*dims, kind=BF16):
        return jax.ShapeDtypeStruct(dims, kind)

    def call(kernel, out_shape, where, inputs, mib, flops, scratch):
        spaces = {"s": pltpu.SMEM, "v": pltpu.VMEM, "h": pltpu.HBM}
        specs = [pl.BlockSpec(memory_space=spaces[w]) for w in where]
        return pl.pallas_call(
            kernel,
            out_shape=out_shape,
            in_specs=specs[: len(inputs)],
            out_specs=tuple(specs[len(inputs) :]),
            scratch_shapes=scratch,
            compiler_params=pltpu.CompilerParams(vmem_limit_bytes=mib * MIB),
            cost_estimate=pl.CostEstimate(flops=flops, bytes_accessed=4 * MIB, transcendentals=0),
        )(*inputs)

    def copies(count):
        return pltpu.SemaphoreType.DMA((count,))

    request = exchange(jnp.concatenate([cold_row[0], cold_bag[0]], axis=1)[:, None, :])
    part_rows = samples + 2 * own_hot + hot_pick.shape[1]
    work = slots * rows * width
    picks = hot_pick.T
    bags = cold_bag.reshape(slots // LANES, LANES)
    (packed,) = call(
        prepare_kernel,
        (shape(part_rows, width),),
        "shhhv",
        [hot_slot, table, dense, picks],
        63,
        work,
        [
            pltpu.VMEM((own_hot, width), F32),
            pltpu.VMEM((samples, width), F32),
            pltpu.VMEM(picks.shape, I32),
            copies(2 + own_hot),
        ],
    )
    chunks = gather_all(packed[None], peers)
    many = "v" * len(chunks)
    (looked,) = call(
        lookup_kernel, (shape(slots, width),), "vvv", [request, table], 24, 2 * work, []
    )
    returned = exchange(looked.reshape(peers, per_peer, width)).reshape(slots, width)
    pooled, err = call(
        pool_kernel,
        (shape(samples, width, kind=F32), shape(peers, 1, samples, kind=F32)),
        "svhhhh" + "h" * len(chunks) + "vv",
        [source, returned, bags, picks, dense, label.reshape(1, samples)] + chunks,
        24,
        work,
        [
            pltpu.VMEM((hot_total, width), BF16),
            pltpu.VMEM((peers, own_hot, width), BF16),
            pltpu.VMEM(bags.shape, I32),
            pltpu.VMEM(picks.shape, I32),
            pltpu.VMEM((samples, width), F32),
            pltpu.VMEM((1, samples), I32),
            copies(4 + len(chunks)),
        ],
    )
    errs = exchange(err)
    early, depth = 4, hot_pick.shape[1]

    def marks(group, order):
        count = sum(chunk.shape[0] for chunk in group)
        return call(
            marks_kernel,
            (
                shape(hot_total // 2, count * samples, kind=jnp.float8_e4m3fn),
                shape(count * per_peer, samples),
                shape(count * per_peer, width),
            ),
            "ssv" + "h" * len(group) + "vvv",
            [order, me[None], request] + group,
            24,
            count * hot_total * samples * depth,
            [
                pltpu.VMEM((count, depth, samples), BF16),
                pltpu.VMEM((count, samples, width), BF16),
                copies(2 * len(group)),
            ],
        )

    ready = sum(chunk.shape[0] for chunk in chunks[:early])
    marks0, cold0, rows0 = marks(chunks[:early], source[:ready])
    marks1, cold1, rows1 = marks(chunks[early:], source[ready:])
    (hot_here,) = call(
        hot_kernel,
        (shape(hot_total // 2, width, kind=F32),),
        "ssvvv" + many + "v",
        [source, me[None], marks0, marks1, errs] + chunks,
        24,
        work,
        [pltpu.VMEM((hot_total // 2, width), F32)],
    )
    hot_there = lax.ppermute(hot_here, AXES, [(i, i ^ 1) for i in range(peers)])
    (new_table,) = call(
        cold_kernel,
        (shape(rows, width, kind=F32),),
        "sssvvvvvvvvv",
        [
            source, hot_slot, me[None], cold0, cold1, rows0, rows1, errs, request, table, hot_here,
        ],
        24,
        4 * work,
        [pltpu.VMEM((slots, width), BF16)],
    )
    split = (peers // 2, 1, own_hot, width)
    here, there = hot_here.reshape(split), hot_there.reshape(split)
    odd = (me & 1) == 1
    hot_new = jnp.concatenate([jnp.where(odd, there, here), jnp.where(odd, here, there)], axis=1)
    hot_new = hot_new.reshape(hot_total, width)
    return (pooled, new_table, hot_new)


def exchanged_body(table, hot_slot, cold_row, cold_bag, hot_pick, dense, label):
    width = table.shape[1]
    samples = dense.shape[0]
    own_hot = hot_slot.shape[0]
    peers, per_peer = cold_row.shape[1], cold_row.shape[2]
    slots = peers * per_peer
    bf16 = BF16
    arrived = exchange(cold_row[0]).reshape(slots)
    rounded = table.astype(bf16)
    owned = jnp.arange(table.shape[0], dtype=jnp.int32)
    looked = rounded[arrived].reshape(peers, per_peer, width)
    hot_rows = table[hot_slot]
    shared = jnp.broadcast_to(hot_rows.astype(bf16)[None], (peers, own_hot, width))
    returned = exchange(jnp.concatenate([looked, shared], axis=1))
    cold_rows = returned[:, :per_peer].reshape(slots, width)
    hot_copy = returned[:, per_peer:].reshape(peers * own_hot, width)
    bags = cold_bag[0].reshape(slots)
    selector = (jnp.arange(samples, dtype=jnp.int32)[:, None] == bags[None, :]).astype(bf16)
    hot_total = peers * own_hot
    picks = jnp.sum(
        (hot_pick[:, :, None] == jnp.arange(hot_total, dtype=jnp.int32)).astype(jnp.float32), axis=1
    ).astype(bf16)
    pooled = jnp.dot(selector, cold_rows, preferred_element_type=jnp.float32) + jnp.dot(
        picks, hot_copy, preferred_element_type=jnp.float32
    )
    score = jnp.sum(pooled * dense, axis=1) / width**0.5
    err = jax.nn.sigmoid(score) - label.astype(jnp.float32)
    grad = (err[:, None] * dense).astype(bf16)
    over_samples = (((0,), (0,)), ((), ()))
    slot_grad = lax.dot_general(selector, grad, over_samples, preferred_element_type=jnp.float32)
    hot_part = lax.dot_general(picks, grad, over_samples, preferred_element_type=jnp.float32)
    sent = jnp.concatenate(
        [
            slot_grad.astype(bf16).reshape(peers, per_peer, width),
            hot_part.astype(bf16).reshape(peers, own_hot, width),
        ],
        axis=1,
    )
    delivered = exchange(sent)
    own_grad = jnp.sum(delivered[:, per_peer:].astype(jnp.float32), axis=0)
    placed = (owned[:, None] == arrived[None, :]).astype(bf16)
    table_grad = jnp.dot(
        placed, delivered[:, :per_peer].reshape(slots, width), preferred_element_type=jnp.float32
    )
    own_new = hot_rows - 0.1 * own_grad
    new_table = (table - 0.1 * table_grad).at[hot_slot].set(own_new)
    hot_new = exchange(jnp.broadcast_to(own_new[None], (peers, own_hot, width)))
    return (pooled, new_table, hot_new.reshape(hot_total, width))


def solution(mesh):
    placed = (
        P(AXES, None),
        P(AXES),
        P(AXES, None, None),
        P(AXES, None, None),
        P(AXES, None),
        P(AXES, None),
        P(AXES),
    )
    devices = mesh.shape["rows"] * mesh.shape["grp"]

    def body(*blocks):
        _, hot_slot, cold_row, _, _, dense, _ = blocks
        samples, own_hot = dense.shape[0], hot_slot.shape[0]
        marks = 2 * devices * samples * devices * own_hot
        fits = marks <= 16 * MIB and 2 * cold_row.shape[2] == LANES
        fits = fits and devices & (devices - 1) == 0 and devices >= 16 and devices * own_hot <= 64 * LANES
        return (gathered_body if fits else exchanged_body)(*blocks)

    return jax.shard_map(
        body,
        mesh=mesh,
        in_specs=placed,
        out_specs=(P(AXES, None), P(AXES, None), P()),
        check_vma=False,
    )
```

```python
import jax
import jax.numpy as jnp
from jax import lax
from jax.experimental import pallas as pl
from jax.experimental.pallas import tpu as pltpu
from jax.sharding import PartitionSpec as P


AXES = ("rows", "grp")
LANES = 128
MIB = 1 << 20
BF16 = jnp.bfloat16
F32 = jnp.float32
I32 = jnp.int32


def exchange(x):
    return lax.all_to_all(x, AXES, split_axis=0, concat_axis=0, tiled=True)


def column(row):
    return jnp.transpose(jnp.broadcast_to(row, (LANES, LANES)))


def lane_iota(shape):
    return lax.broadcasted_iota(I32, shape, 1)


def one_hot(mask):
    return jnp.where(mask, 1.0, 0.0).astype(BF16)


def packed_row(ref, at, per_peer, part):
    row = None
    for j in range(LANES // per_peer):
        shift = (j - part) * per_peer % LANES
        other = ref[at(j)]
        other = pltpu.roll(other, shift, 1) if shift else other
        row = other if row is None else jnp.where(lane_iota(row.shape) < j * per_peer, row, other)
    return row


def mark_of(ids):
    return ((LANES + (ids & (LANES - 1))) << (ids >> 7)).astype(F32).astype(BF16)


def fetch(pairs, sems):
    copies = [pltpu.make_async_copy(a, b, sems.at[k]) for k, (a, b) in enumerate(pairs)]
    for copy in copies:
        copy.start()
    return copies


def offsets(chunks):
    return [sum(chunk.shape[0] for chunk in chunks[:k]) for k in range(len(chunks))]


def prepare_kernel(
    slot_ref, table_hbm, dense_hbm, pick_hbm, packed_ref, hot_ref, dense_ref, pick_ref, sems
):
    own_hot = slot_ref.shape[0]
    dense_in, pick_in, *rows_in = fetch(
        [(dense_hbm, dense_ref), (pick_hbm, pick_ref)]
        + [
            (table_hbm.at[pl.ds(slot_ref[k], 1)], hot_ref.at[pl.ds(k, 1)])
            for k in range(own_hot)
        ],
        sems,
    )
    samples = dense_ref.shape[0]
    dense_in.wait()
    packed_ref[:samples, :] = dense_ref[...].astype(BF16)
    pick_in.wait()
    packed_ref[samples + 2 * own_hot :, :] = mark_of(pick_ref[...])
    for row_in in rows_in:
        row_in.wait()
    hot = hot_ref[...]
    high = hot.astype(BF16)
    packed_ref[samples : samples + own_hot, :] = high
    packed_ref[samples + own_hot : samples + 2 * own_hot, :] = (hot - high.astype(F32)).astype(BF16)


def lookup_kernel(request_ref, table_ref, out_ref):
    peers = request_ref.shape[0]
    rows = table_ref.shape[0]
    per_peer = request_ref.shape[2] // 2
    group = LANES // per_peer
    tile = 4
    table = table_ref[...].astype(BF16)
    for first in range(0, peers // group, tile):
        pieces = []
        for k in range(first, first + tile):
            wanted = column(packed_row(request_ref, lambda j: k * group + j, per_peer, 0))
            pieces.append(
                jnp.concatenate(
                    [one_hot(wanted == lane_iota(wanted.shape) + c) for c in range(0, rows, LANES)],
                    axis=1,
                )
            )
        hits = jnp.concatenate(pieces, axis=0)
        out_ref[first * LANES : (first + tile) * LANES, :] = jnp.dot(
            hits, table, preferred_element_type=F32
        ).astype(BF16)


def marks_kernel(source_ref, me_ref, request_ref, *refs):
    *chunks, hot_ref, cold_ref, rows_ref, pick_ref, dense_ref, sems = refs
    per_peer = request_ref.shape[2] // 2
    samples = cold_ref.shape[1]
    own_hot = 2 * hot_ref.shape[0] // request_ref.shape[0]
    first = samples + 2 * own_hot
    picks_in = fetch(
        [
            (chunk.at[:, first:], pick_ref.at[pl.ds(n, chunk.shape[0])])
            for n, chunk in zip(offsets(chunks), chunks)
        ],
        sems,
    )
    dense_in = fetch(
        [
            (chunk.at[:, :samples], dense_ref.at[pl.ds(n, chunk.shape[0])])
            for n, chunk in zip(offsets(chunks), chunks)
        ],
        sems.at[pl.ds(len(chunks), len(chunks))],
    )
    one, zero = jnp.ones((), BF16), jnp.zeros((), BF16)
    for n in range(pick_ref.shape[0]):
        bags = column(request_ref[source_ref[n]])[per_peer:]
        at = n * per_peer
        for c in range(0, samples, LANES):
            cold_ref[at : at + per_peer, c : c + LANES] = one_hot(bags == lane_iota(bags.shape) + c)
    rows = lax.broadcasted_iota(I32, (hot_ref.shape[0], LANES), 0)
    odd = me_ref[0] & 1
    ids = mark_of(rows + (rows // own_hot + odd) * own_hot)
    for arrived in picks_in:
        arrived.wait()
    for n in range(pick_ref.shape[0]):
        for c in range(0, samples, LANES):
            total = None
            for j in range(pick_ref.shape[1]):
                hit = jnp.where(ids == pick_ref[n, j : j + 1, c : c + LANES], one, zero)
                total = hit if total is None else total + hit
            at = n * samples + c
            hot_ref[:, at : at + LANES] = total.astype(hot_ref.dtype)
    for arrived in dense_in:
        arrived.wait()
    for n in range(pick_ref.shape[0]):
        at = slice(n * per_peer, (n + 1) * per_peer)
        rows_ref[at, :] = jnp.dot(
            cold_ref[at, :], dense_ref[n], preferred_element_type=F32
        ).astype(BF16)


def pool_kernel(source_ref, rows_ref, bag_hbm, pick_hbm, dense_hbm, label_hbm, *refs):
    *chunks, pooled_ref, err_ref, hot_ref, near_ref, bag_ref, pick_ref, dense_ref, label_ref, sems = refs
    samples, width = dense_ref.shape
    hot_total = hot_ref.shape[0]
    own_hot = hot_total // err_ref.shape[0]
    high = slice(samples, samples + own_hot)
    bag_in, pick_in, dense_in, label_in, *hot_in = fetch(
        [
            (bag_hbm, bag_ref),
            (pick_hbm, pick_ref),
            (dense_hbm, dense_ref),
            (label_hbm, label_ref),
        ]
        + [
            (chunk.at[:, high], near_ref.at[pl.ds(n, chunk.shape[0])])
            for n, chunk in zip(offsets(chunks), chunks)
        ],
        sems,
    )
    bag_in.wait()
    ids = lax.broadcasted_iota(I32, (samples, LANES), 0)
    chosen = jnp.concatenate(
        [one_hot(ids == bag_ref[k : k + 1, :]) for k in range(bag_ref.shape[0])], axis=1
    )
    pooled = jnp.dot(chosen, rows_ref[...], preferred_element_type=F32)
    pick_in.wait()
    counts = []
    for h in range(0, hot_total, LANES):
        ids = lax.broadcasted_iota(I32, (LANES, samples), 0) + h
        total = jnp.zeros((LANES, samples), F32)
        for j in range(pick_ref.shape[0]):
            total = total + jnp.where(ids == pick_ref[j : j + 1, :], 1.0, 0.0)
        counts.append(total.astype(BF16))
    for arrived in hot_in:
        arrived.wait()
    for n in range(near_ref.shape[0]):
        at = pl.multiple_of(source_ref[n] * own_hot, own_hot)
        hot_ref[pl.ds(at, own_hot), :] = near_ref[n]
    pooled = pooled + lax.dot_general(
        jnp.concatenate(counts, axis=0),
        hot_ref[...],
        (((0,), (0,)), ((), ())),
        preferred_element_type=F32,
    )
    pooled_ref[...] = pooled
    dense_in.wait()
    label_in.wait()
    score = jnp.sum(pooled * dense_ref[...], axis=1, keepdims=True) / width**0.5
    flat = jnp.transpose(jnp.broadcast_to(score, (samples, LANES)))[:1, :]
    err = 1.0 / (1.0 + jnp.exp(-flat)) - label_ref[...].astype(F32)
    err_ref[...] = jnp.broadcast_to(err[None], err_ref.shape)


def hot_kernel(source_ref, me_ref, marks0_ref, marks1_ref, err_ref, *refs):
    *chunks, new_ref, grad_ref = refs
    hot_half, _ = new_ref.shape
    peers = err_ref.shape[0]
    samples = err_ref.shape[2]
    own_hot = 2 * hot_half // peers
    total, n = None, 0
    for chunk in chunks:
        parts = chunk.shape[0]
        errs = [err_ref[source_ref[n + p]].astype(BF16) for p in range(parts)]
        marks_ref, at = marks0_ref, n * samples
        if at >= marks0_ref.shape[1]:
            marks_ref, at = marks1_ref, at - marks0_ref.shape[1]
        near = jnp.dot(
            marks_ref[:, at : at + parts * samples].astype(BF16) * jnp.concatenate(errs, axis=1),
            jnp.concatenate([chunk[p, :samples, :] for p in range(parts)], axis=0),
            preferred_element_type=F32,
        )
        total = near if total is None else total + near
        n += parts
    grad_ref[...] = total
    odd = me_ref[0] & 1
    n = 0
    for chunk in chunks:
        for p in range(chunk.shape[0]):
            owner = source_ref[n]

            @pl.when((owner & 1) == odd)
            def _():
                at = pl.multiple_of((owner // 2) * own_hot, own_hot)
                old = chunk[p, samples : samples + own_hot, :].astype(F32)
                old = old + chunk[p, samples + own_hot : samples + 2 * own_hot, :].astype(F32)
                new_ref[pl.ds(at, own_hot), :] = old - 0.1 * grad_ref[pl.ds(at, own_hot), :]

            n += 1


def cold_kernel(
    source_ref, slot_ref, me_ref, cold0_ref, cold1_ref, rows0_ref, rows1_ref, err_ref, request_ref,
    table_ref, hot_ref, new_hbm, slots_ref, new_ref, sems,
):
    rows = table_ref.shape[0]
    peers = request_ref.shape[0]
    per_peer = request_ref.shape[2] // 2
    own_hot = slot_ref.shape[0]
    early = cold0_ref.shape[0] // per_peer
    for n in range(peers):
        cold_ref, rows_ref, at = cold0_ref, rows0_ref, n * per_peer
        if n >= early:
            cold_ref, rows_ref, at = cold1_ref, rows1_ref, (n - early) * per_peer
        err = cold_ref[at : at + per_peer, :].astype(F32) * err_ref[source_ref[n]]
        err = jnp.sum(err, axis=1, keepdims=True)
        slots_ref[n * per_peer : (n + 1) * per_peer, :] = (
            err * rows_ref[at : at + per_peer, :].astype(F32)
        ).astype(BF16)
    group = LANES // per_peer
    packed = [
        packed_row(request_ref, lambda j: source_ref[n + j], per_peer, 0)
        for n in range(0, peers, group)
    ]
    chunk_rows, block = 256, rows // sems.shape[0]
    ids = lax.broadcasted_iota(I32, (chunk_rows, LANES), 0)
    base = (me_ref[0] // 2) * own_hot
    outs = []
    for k in range(sems.shape[0]):
        for r in range(k * block, (k + 1) * block, chunk_rows):
            place = jnp.concatenate([one_hot(ids + r == row) for row in packed], axis=1)
            moved = jnp.dot(place, slots_ref[...], preferred_element_type=F32)
            new_ref[r : r + chunk_rows, :] = table_ref[r : r + chunk_rows, :] - 0.1 * moved
        for j in range(own_hot):
            slot = slot_ref[j]

            @pl.when((slot >= k * block) & (slot < (k + 1) * block))
            def _():
                new_ref[pl.ds(slot, 1), :] = hot_ref[pl.ds(base + j, 1), :]

        here = slice(k * block, (k + 1) * block)
        outs += fetch([(new_ref.at[here], new_hbm.at[here])], sems.at[pl.ds(k, 1)])
    for out in outs:
        out.wait()


def gather_all(x, devices):
    def swap(held, mask):
        return lax.ppermute(held, AXES, [(i, i ^ mask(i)) for i in range(devices)])

    first = lambda i: 2 if i & 1 else 4
    second = lambda i: 4 if i & 1 else 2
    other = lambda i: 1
    deep = [swap(x, lambda i: mask) for mask in deep_masks(devices)]
    near = [x, swap(x, first), swap(x, second)]
    near = jnp.concatenate(near + [swap(near[1], second)], axis=0)
    own = jnp.concatenate(deep, axis=0)
    across = swap(own, first)
    up = swap(own, second)
    held = [near, own, across, up, swap(across, second)]
    return held + [swap(chunk, other) for chunk in held]


def deep_masks(devices):
    masks = [0]
    for b in range(devices.bit_length() - 2, 2, -1):
        masks += [mask | 1 << b for mask in masks]
    return masks[1:]


def sources_of(me, devices):
    deep = deep_masks(devices)

    def half(owner):
        first = jnp.where(owner & 1 == 1, 2, 4)
        turns = [0, first, 6 - first, 6]
        return [owner ^ turn for turn in turns] + [owner ^ turn ^ m for turn in turns for m in deep]

    return jnp.stack(half(me) + half(me ^ 1)).astype(I32)


def gathered_body(table, hot_slot, cold_row, cold_bag, hot_pick, dense, label):
    rows, width = table.shape
    samples = dense.shape[0]
    own_hot = hot_slot.shape[0]
    peers, per_peer = cold_row.shape[1], cold_row.shape[2]
    slots = peers * per_peer
    hot_total = peers * own_hot
    me = lax.axis_index(AXES).astype(I32)
    source = sources_of(me, peers)

    def shape(*dims, kind=BF16):
        return jax.ShapeDtypeStruct(dims, kind)

    def call(kernel, out_shape, where, inputs, mib, flops, scratch):
        spaces = {"s": pltpu.SMEM, "v": pltpu.VMEM, "h": pltpu.HBM}
        specs = [pl.BlockSpec(memory_space=spaces[w]) for w in where]
        return pl.pallas_call(
            kernel,
            out_shape=out_shape,
            in_specs=specs[: len(inputs)],
            out_specs=tuple(specs[len(inputs) :]),
            scratch_shapes=scratch,
            compiler_params=pltpu.CompilerParams(vmem_limit_bytes=mib * MIB),
            cost_estimate=pl.CostEstimate(flops=flops, bytes_accessed=4 * MIB, transcendentals=0),
        )(*inputs)

    def copies(count):
        return pltpu.SemaphoreType.DMA((count,))

    request = exchange(jnp.concatenate([cold_row[0], cold_bag[0]], axis=1)[:, None, :])
    part_rows = samples + 2 * own_hot + hot_pick.shape[1]
    work = slots * rows * width
    picks = hot_pick.T
    bags = cold_bag.reshape(slots // LANES, LANES)
    (packed,) = call(
        prepare_kernel,
        (shape(part_rows, width),),
        "shhhv",
        [hot_slot, table, dense, picks],
        63,
        work,
        [
            pltpu.VMEM((own_hot, width), F32),
            pltpu.VMEM((samples, width), F32),
            pltpu.VMEM(picks.shape, I32),
            copies(2 + own_hot),
        ],
    )
    chunks = gather_all(packed[None], peers)
    many = "v" * len(chunks)
    (looked,) = call(
        lookup_kernel, (shape(slots, width),), "vvv", [request, table], 24, 2 * work, []
    )
    returned = exchange(looked.reshape(peers, per_peer, width)).reshape(slots, width)
    pooled, err = call(
        pool_kernel,
        (shape(samples, width, kind=F32), shape(peers, 1, samples, kind=F32)),
        "svhhhh" + "h" * len(chunks) + "vv",
        [source, returned, bags, picks, dense, label.reshape(1, samples)] + chunks,
        24,
        work,
        [
            pltpu.VMEM((hot_total, width), BF16),
            pltpu.VMEM((peers, own_hot, width), BF16),
            pltpu.VMEM(bags.shape, I32),
            pltpu.VMEM(picks.shape, I32),
            pltpu.VMEM((samples, width), F32),
            pltpu.VMEM((1, samples), I32),
            copies(4 + len(chunks)),
        ],
    )
    errs = exchange(err)
    early, depth = 4, hot_pick.shape[1]

    def marks(group, order):
        count = sum(chunk.shape[0] for chunk in group)
        return call(
            marks_kernel,
            (
                shape(hot_total // 2, count * samples, kind=jnp.float8_e4m3fn),
                shape(count * per_peer, samples),
                shape(count * per_peer, width),
            ),
            "ssv" + "h" * len(group) + "vvv",
            [order, me[None], request] + group,
            24,
            count * hot_total * samples * depth,
            [
                pltpu.VMEM((count, depth, samples), BF16),
                pltpu.VMEM((count, samples, width), BF16),
                copies(2 * len(group)),
            ],
        )

    ready = sum(chunk.shape[0] for chunk in chunks[:early])
    marks0, cold0, rows0 = marks(chunks[:early], source[:ready])
    marks1, cold1, rows1 = marks(chunks[early:], source[ready:])
    (hot_here,) = call(
        hot_kernel,
        (shape(hot_total // 2, width, kind=F32),),
        "ssvvv" + many + "v",
        [source, me[None], marks0, marks1, errs] + chunks,
        24,
        work,
        [pltpu.VMEM((hot_total // 2, width), F32)],
    )
    hot_there = lax.ppermute(hot_here, AXES, [(i, i ^ 1) for i in range(peers)])
    (new_table,) = call(
        cold_kernel,
        (shape(rows, width, kind=F32),),
        "sssvvvvvvvvh",
        [
            source, hot_slot, me[None], cold0, cold1, rows0, rows1, errs, request, table, hot_here,
        ],
        24,
        4 * work,
        [pltpu.VMEM((slots, width), BF16), pltpu.VMEM((rows, width), F32), copies(4)],
    )
    split = (peers // 2, 1, own_hot, width)
    here, there = hot_here.reshape(split), hot_there.reshape(split)
    odd = (me & 1) == 1
    hot_new = jnp.concatenate([jnp.where(odd, there, here), jnp.where(odd, here, there)], axis=1)
    hot_new = hot_new.reshape(hot_total, width)
    return (pooled, new_table, hot_new)


def exchanged_body(table, hot_slot, cold_row, cold_bag, hot_pick, dense, label):
    width = table.shape[1]
    samples = dense.shape[0]
    own_hot = hot_slot.shape[0]
    peers, per_peer = cold_row.shape[1], cold_row.shape[2]
    slots = peers * per_peer
    bf16 = BF16
    arrived = exchange(cold_row[0]).reshape(slots)
    rounded = table.astype(bf16)
    owned = jnp.arange(table.shape[0], dtype=jnp.int32)
    looked = rounded[arrived].reshape(peers, per_peer, width)
    hot_rows = table[hot_slot]
    shared = jnp.broadcast_to(hot_rows.astype(bf16)[None], (peers, own_hot, width))
    returned = exchange(jnp.concatenate([looked, shared], axis=1))
    cold_rows = returned[:, :per_peer].reshape(slots, width)
    hot_copy = returned[:, per_peer:].reshape(peers * own_hot, width)
    bags = cold_bag[0].reshape(slots)
    selector = (jnp.arange(samples, dtype=jnp.int32)[:, None] == bags[None, :]).astype(bf16)
    hot_total = peers * own_hot
    picks = jnp.sum(
        (hot_pick[:, :, None] == jnp.arange(hot_total, dtype=jnp.int32)).astype(jnp.float32), axis=1
    ).astype(bf16)
    pooled = jnp.dot(selector, cold_rows, preferred_element_type=jnp.float32) + jnp.dot(
        picks, hot_copy, preferred_element_type=jnp.float32
    )
    score = jnp.sum(pooled * dense, axis=1) / width**0.5
    err = jax.nn.sigmoid(score) - label.astype(jnp.float32)
    grad = (err[:, None] * dense).astype(bf16)
    over_samples = (((0,), (0,)), ((), ()))
    slot_grad = lax.dot_general(selector, grad, over_samples, preferred_element_type=jnp.float32)
    hot_part = lax.dot_general(picks, grad, over_samples, preferred_element_type=jnp.float32)
    sent = jnp.concatenate(
        [
            slot_grad.astype(bf16).reshape(peers, per_peer, width),
            hot_part.astype(bf16).reshape(peers, own_hot, width),
        ],
        axis=1,
    )
    delivered = exchange(sent)
    own_grad = jnp.sum(delivered[:, per_peer:].astype(jnp.float32), axis=0)
    placed = (owned[:, None] == arrived[None, :]).astype(bf16)
    table_grad = jnp.dot(
        placed, delivered[:, :per_peer].reshape(slots, width), preferred_element_type=jnp.float32
    )
    own_new = hot_rows - 0.1 * own_grad
    new_table = (table - 0.1 * table_grad).at[hot_slot].set(own_new)
    hot_new = exchange(jnp.broadcast_to(own_new[None], (peers, own_hot, width)))
    return (pooled, new_table, hot_new.reshape(hot_total, width))


def solution(mesh):
    placed = (
        P(AXES, None),
        P(AXES),
        P(AXES, None, None),
        P(AXES, None, None),
        P(AXES, None),
        P(AXES, None),
        P(AXES),
    )
    devices = mesh.shape["rows"] * mesh.shape["grp"]

    def body(*blocks):
        _, hot_slot, cold_row, _, _, dense, _ = blocks
        samples, own_hot = dense.shape[0], hot_slot.shape[0]
        marks = 2 * devices * samples * devices * own_hot
        fits = marks <= 16 * MIB and 2 * cold_row.shape[2] == LANES
        fits = fits and devices & (devices - 1) == 0 and devices >= 16 and devices * own_hot <= 64 * LANES
        return (gathered_body if fits else exchanged_body)(*blocks)

    return jax.shard_map(
        body,
        mesh=mesh,
        in_specs=placed,
        out_specs=(P(AXES, None), P(AXES, None), P()),
        check_vma=False,
    )
```
